32 devices in a mesh: dp: 4 (over y, x), expert: 8 (over z, core).
Axes of the slice: x: 2, y: 2, z: 4, core: 2. Of those that a mesh axis runs over, the one named last changes fastest.
Arguments:
- expert_down: bfloat16 [3072, 2048], P('expert'), may hold values from -0.125 to 0.125
- out_grad: bfloat16 [4096, 2048], P(('dp', 'expert')), parts along dimension 0, may hold values from -6 to 6
- routes: int32 [4096, 2], P(('dp', 'expert')), parts along dimension 0, may hold values from 0 to 3, all different within a row; in each aligned block of 128 rows (0 to 127, 128 to 255, ...) at most 96 rows name the same one
- gates: float32 [4096, 2], P(('dp', 'expert')), parts along dimension 0, may hold values from 0.1 to 1
Outputs:
- hidden_grad: bfloat16 [4096, 2, 768], P(('dp', 'expert')), parts along dimension 0
The draws below stay inside these ranges and needn't reach their ends.
There are 4 independent parts, one for each index of `dp`. The reference program is written for one: setup_inputs(seed, part) draws one part's arguments, and reference() takes and returns one part's arrays. A program takes and returns all parts, laid end to end along the dimension named above; an argument that names none is the same for every part. Nothing has to cross between parts.
Inputs may be any that keep to these rules, and one draw needn't show every extreme that they name: `routes`: each token names 2 different experts; among the 128 tokens of one device no expert is named more than 96 times.
All inputs are finite; a program needn't handle non-finite values.
Results may differ from the reference program's by a relative error of at most 0.0049.
Values may be sent and summed in bfloat16 or wider, within the bound.
No kernel may reach another device: no remote copies, remote signals or barrier semaphores. Data moves between devices by JAX's collectives and lax.ppermute only.
A program may use at most 64 MiB of HBM per device.

```python
import math
import jax
import jax.numpy as jnp
import numpy as np
from jax import lax

D = 2048
FF = 768
TOK_DEV = 128
EXPERTS = 4
TOP = 2
CAP = 96
TOKENS = 1024
N_EXPERT = 8


def shard_levels(rng, dims, shards, least, largest):
    gain, own = 1.0, jax.random.fold_in(rng, 6)
    for axis_at, shards_of in shards:
        heights = jnp.exp(jax.random.uniform(jax.random.fold_in(own, axis_at), (shards_of,), jnp.float32, least / len(shards), largest / len(shards)))
        gain = gain * jnp.repeat(heights, dims[axis_at] // shards_of).reshape([-1 if axis == axis_at else 1 for axis in range(len(dims))])
    return gain


def assign_block(rng, own, number, rows, number_of, top, most, lean):
    ranking = jax.random.permutation(rng, number_of)
    packed, ordinary = shares(number_of, rows * top, most, lean, True), shares(number_of, rows * top, most, lean, False)
    places = jnp.arange(number_of)

    def named(lengths, rotation):
        used = int((lengths > 0).sum())
        fixed = max(1, used // 4)
        moved = fixed + (places - fixed + rotation * (used - fixed)) % max(1, number_of - fixed)
        return jnp.zeros((number_of,), jnp.int32).at[ranking[jnp.where(places < fixed, places, moved)]].set(jnp.asarray(lengths, jnp.int32))

    lengths = jnp.where(number % 4 == 0, named(packed, number // 4), named(ordinary, number - number // 4 - 1))
    mixed = jax.random.permutation(jax.random.fold_in(own, 3), number_of)
    source_of, sink = mixed[0:number_of // 2 * 2:2], mixed[1:number_of // 2 * 2:2]
    slack = jnp.minimum(lengths[source_of] - 1, most - lengths[sink]) // 2
    slack = jnp.where((source_of == ranking[0]) | (sink == ranking[0]) | (lengths[sink] == 0), 0, jnp.maximum(slack, 0))
    moved = jax.random.randint(jax.random.fold_in(own, 4), (number_of // 2,), 0, 1 << 20) % (slack + 1)
    lengths = lengths.at[source_of].add(-moved).at[sink].add(moved)
    items = jnp.searchsorted(jnp.cumsum(lengths), jnp.arange(rows * top), side="right").astype(jnp.int32)
    listing = items.reshape(top, rows).T
    listing = listing[jax.random.permutation(jax.random.fold_in(own, 1), rows)]
    rotation = jax.random.randint(jax.random.fold_in(own, 2), (rows, 1), 0, top)
    return jnp.take_along_axis(listing, (jnp.arange(top)[None, :] + rotation) % top, axis=1)


def shares(amount, total, bound, slope, full):
    loads = [(1 << 20) // math.isqrt(grade ** slope) + 1 for grade in range(1, amount + 1)]
    largest = bound if full else min(bound, max(-(-total // amount), total * loads[0] // sum(loads)))
    least = 1 if total - largest >= amount - 1 else 0
    given, spare = [largest] + [least] * (amount - 1), total - largest - least * (amount - 1)
    while spare > 0:
        movable = [i for i in range(1, amount) if given[i] < largest] or [i for i in range(1, amount) if given[i] < bound]
        mass, budget = sum([loads[i] for i in movable]), spare
        for i in movable:
            extra = min(bound - given[i], max(1, budget * loads[i] // mass), spare)
            given[i] = given[i] + extra
            spare = spare - extra
    return np.array(given)


def centred(key, shape, width, most, cuts=(), held_as=jnp.bfloat16):
    array = jax.random.normal(key, shape, jnp.float32) * width
    if len(cuts) > 0:
        array = shard_levels(key, shape, cuts, -0.22, 0.18) * array
    return jnp.clip(array, min=-most, max=most).astype(held_as)


def setup_inputs(seed: int = 0, part: int = 0) -> dict:
    splits = jax.random.split(jax.random.key(seed), 5)
    own_keys = jax.random.split(jax.random.fold_in(splits[4], part), 5)
    expert_down = centred(splits[0], (EXPERTS * FF, D), D ** -0.5, 0.125, ((0, 8),))
    out_grad = centred(own_keys[1], (TOKENS, D), 1.0, 6.0, ((0, 8),))
    routes_keys = jax.random.split(jax.random.fold_in(own_keys[2], 1), TOKENS // TOK_DEV)
    routes_turns = jax.random.permutation(jax.random.fold_in(own_keys[2], 3), TOKENS // TOK_DEV)
    routes = jax.vmap(lambda own, number: assign_block(jax.random.fold_in(own_keys[2], 2), own, number, TOK_DEV, EXPERTS, TOP, CAP, 2))(routes_keys, routes_turns).reshape((TOKENS, TOP))
    gates = jnp.clip(0.1 + 0.9 * jax.random.uniform(own_keys[3], (TOKENS, TOP), jnp.float32) ** shard_levels(own_keys[3], (TOKENS, TOP), ((0, 8),), -0.2, 0.2), 0.1, 1.0)
    return dict(expert_down=expert_down, out_grad=out_grad, routes=routes, gates=gates)


def block_slots(expert_ids):
    one_hot = (expert_ids[:, None] == jnp.arange(EXPERTS, dtype=jnp.int32)[None, :]).astype(jnp.int32)
    earlier = jnp.cumsum(one_hot, axis=0) - one_hot
    return jnp.sum(earlier * one_hot, axis=1).astype(jnp.int32)


def reference(expert_down, out_grad, routes, gates):
    per_block = TOK_DEV * TOP
    expert_ids = routes.reshape(N_EXPERT, per_block).astype(jnp.int32)
    slots = jax.vmap(block_slots)(expert_ids)
    block_index = jnp.arange(N_EXPERT, dtype=jnp.int32)[:, None]
    source_token = (jnp.arange(per_block, dtype=jnp.int32) // TOP)[None, :] + block_index * TOK_DEV
    position = (expert_ids * (N_EXPERT * CAP) + block_index * CAP + slots).reshape(-1)
    token_table = jnp.zeros((EXPERTS * N_EXPERT * CAP,), jnp.int32).at[position].set(source_token.reshape(-1))
    token_table = token_table.reshape(EXPERTS, N_EXPERT * CAP)
    weights = expert_down.reshape(EXPERTS, FF, D)

    def per_expert(operands):
        rows_index, weight = operands
        routed_rows = out_grad[rows_index]
        return jnp.dot(routed_rows, weight.T, preferred_element_type=jnp.float32).astype(jnp.bfloat16)

    partial_value = lax.map(per_expert, (token_table, weights))
    picked = partial_value.reshape(EXPERTS * N_EXPERT * CAP, FF)[position]
    result = (gates.reshape(-1)[:, None] * picked.astype(jnp.float32)).astype(jnp.bfloat16)
    return result.reshape(TOKENS, TOP, FF)
```

```python
import functools

import jax
import jax.numpy as jnp
from jax import lax
from jax.experimental import pallas as pl
from jax.experimental.pallas import tpu as pltpu
from jax.sharding import PartitionSpec as P


def swapped_2(value, axis, apart):
    mask = 2**apart
    pairs = [(source, source ^ mask) for source in range(lax.axis_size(axis))]
    return lax.ppermute(value, axis, pairs)


def slot_table(routes, experts, capacity):
    local_tokens, choices = routes.shape
    expert_ids = routes.reshape(-1)
    one_hot = (expert_ids[:, None] == jnp.arange(experts, dtype=jnp.int32)[None, :]).astype(
        jnp.int32
    )
    earlier = jnp.cumsum(one_hot, axis=0) - one_hot
    slots = jnp.sum(earlier * one_hot, axis=1)
    position = expert_ids * capacity + slots
    source_token = jnp.arange(local_tokens * choices, dtype=jnp.int32) // choices
    token_table = jnp.zeros((experts * capacity,), jnp.int32).at[position].set(source_token)
    return (expert_ids, slots, token_table.reshape(experts, capacity))


def contract_width(rows, weight):
    return lax.dot_general(
        rows, weight, (((2,), (1,)), ((), ())), preferred_element_type=jnp.float32
    )


def slot_shards(expert_down, out_grad, routes, gates):
    devices = lax.axis_size("expert")
    experts = devices // 2
    local_tokens, choices = routes.shape
    hidden_half = expert_down.shape[0]
    capacity = 3 * local_tokens * choices // (2 * experts)
    expert_ids, slots, token_table = slot_table(routes, experts, capacity)
    parity = lax.axis_index("expert") % 2
    swapped = swapped_2(expert_down, "expert", 0)
    first_rows = jnp.where(parity == 0, expert_down, swapped)
    second_rows = jnp.where(parity == 0, swapped, expert_down)
    half_capacity = capacity // 2
    dispatch_order = token_table.reshape(experts, half_capacity, 2).transpose(0, 2, 1)
    outgoing = out_grad[dispatch_order.reshape(devices, half_capacity)]
    arrived = lax.all_to_all(outgoing, "expert", split_axis=0, concat_axis=0, tiled=True)
    low_part = contract_width(arrived, first_rows).astype(jnp.bfloat16)
    high_part = contract_width(arrived, second_rows).astype(jnp.bfloat16)
    product = jnp.concatenate([low_part, high_part], axis=2)
    returned = lax.all_to_all(product, "expert", split_axis=0, concat_axis=0, tiled=True)
    picked = returned.reshape(experts, 2, half_capacity, 2 * hidden_half)[
        expert_ids, slots % 2, slots // 2, :
    ]
    result = (gates.reshape(-1)[:, None] * picked.astype(jnp.float32)).astype(jnp.bfloat16)
    return result.reshape(local_tokens, choices, 2 * hidden_half)


VMEM = pltpu.VMEM


def project(tokens, low, high):
    rows = jnp.concatenate([low, high], axis=0)
    value = lax.dot_general(tokens, rows, (((1,), (1,)), ((), ())), preferred_element_type=jnp.float32)
    return value.astype(jnp.bfloat16)


def keep_chosen(routes, expert, value, kept):
    choices = routes.shape[1]
    width = value.shape[1]
    parts = [
        jnp.where(routes[:, j : j + 1] == expert, value, kept[:, j * width : (j + 1) * width])
        for j in range(choices)
    ]
    return jnp.concatenate(parts, axis=1)


def multiply_body(groups, slots, has_kept, *refs):
    ids_ref = refs[0]
    token_refs = refs[1 : 1 + groups]
    route_refs = refs[1 + groups : 1 + 2 * groups]
    at = 1 + 2 * groups
    weight_refs = refs[at : at + 2 * slots]
    at += 2 * slots
    kept_refs = refs[at : at + groups] if has_kept else None
    at += groups if has_kept else 0
    out_refs = refs[at : at + groups]
    for g in range(groups):
        kept = kept_refs[g][...] if has_kept else jnp.zeros(out_refs[g].shape, jnp.bfloat16)
        for s in range(slots):
            value = project(token_refs[g][...], weight_refs[2 * s][...], weight_refs[2 * s + 1][...])
            kept = keep_chosen(route_refs[g][...], ids_ref[s], value, kept)
        out_refs[g][...] = kept


def multiply(ids, tokens, routes, weights, kept=None):
    groups, slots = len(tokens), len(weights)
    rows, width = tokens[0].shape
    piece = weights[0][0].shape[0]
    choices = routes[0].shape[1]
    operands = [ids, *tokens, *routes]
    for low, high in weights:
        operands += [low, high]
    if kept is not None:
        operands += kept
    shape = jax.ShapeDtypeStruct((rows, choices * 2 * piece), jnp.bfloat16)
    return pl.pallas_call(
        functools.partial(multiply_body, groups, slots, kept is not None),
        out_shape=[shape] * groups,
        in_specs=[pl.BlockSpec(memory_space=pltpu.SMEM)]
        + [pl.BlockSpec(memory_space=VMEM)] * (len(operands) - 1),
        out_specs=[pl.BlockSpec(memory_space=VMEM)] * groups,
        cost_estimate=pl.CostEstimate(
            flops=2 * groups * rows * slots * 2 * piece * width,
            bytes_accessed=2 * (groups * rows * width + slots * 2 * piece * width),
            transcendentals=0,
        ),
        name=f"multiply_{slots}_{'late' if kept is not None else 'early'}",
    )(*operands)


def piece_shards(expert_down, out_grad, routes, gates):
    devices = lax.axis_size("expert")
    replicas = lax.axis_size("dp")
    chips = devices // 2
    local_tokens, choices = routes.shape
    hidden_half, width = expert_down.shape
    piece = hidden_half // replicas
    replica = lax.axis_index("dp")
    place = lax.axis_index("expert")
    chip, core = place // 2, place % 2

    def along(value, by):
        return lax.ppermute(value, "expert", [(i, (i + 2 * by) % devices) for i in range(devices)])

    def other_core(value):
        return lax.ppermute(value, "expert", [(i, i ^ 1) for i in range(devices)])

    def other_replica(value, mask):
        return lax.ppermute(value, "dp", [(i, i ^ mask) for i in range(replicas)])

    mine = lax.dynamic_slice(expert_down, (replica * piece, 0), (piece, width))
    ups, downs = [mine], [mine]
    for _ in range(chips // 2):
        ups.append(along(ups[-1], 1))
    for _ in range((chips - 1) // 2):
        downs.append(along(downs[-1], -1))
    held = [(mine, chip)]
    for step in range(1, chips // 2 + 1):
        if step < len(downs):
            held.append((downs[step], (chip + step) % chips))
        held.append((ups[step], (chip - step) % chips))
    weights = [(rows, other_core(rows)) for rows, _ in held]
    ids = jnp.stack([expert for _, expert in held]).astype(jnp.int32)

    tokens = [out_grad] + [other_replica(out_grad, mask) for mask in range(1, replicas)]
    named = [routes] + [other_replica(routes, mask) for mask in range(1, replicas)]
    early = multiply(ids[:-1], tokens, named, weights[:-1])
    late = multiply(ids[-1:], tokens, named, weights[-1:], early)
    back = [late[0]] + [other_replica(late[mask], mask) for mask in range(1, replicas)]

    stacked = jnp.stack(back)
    ordered = stacked[jnp.arange(replicas) ^ replica]
    ordered = ordered.reshape(replicas, local_tokens, choices, 2, piece)
    ordered = jnp.where(core == 0, ordered, ordered[:, :, :, ::-1])
    picked = ordered.transpose(1, 2, 3, 0, 4).reshape(local_tokens, choices, 2 * hidden_half)
    return (gates[:, :, None] * picked.astype(jnp.float32)).astype(jnp.bfloat16)


def shards(expert_down, out_grad, routes, gates):
    experts, replicas = lax.axis_size("expert") // 2, lax.axis_size("dp")
    shared = experts <= replicas and replicas & (replicas - 1) == 0
    shared = shared and expert_down.shape[0] % (16 * replicas) == 0
    plan = piece_shards if shared else slot_shards
    return plan(expert_down, out_grad, routes, gates)


def solution(mesh):
    placed = (
        P("expert", None),
        P(("dp", "expert"), None),
        P(("dp", "expert"), None),
        P(("dp", "expert"), None),
    )
    return jax.shard_map(
        shards,
        mesh=mesh,
        in_specs=placed,
        out_specs=P(("dp", "expert"), None, None),
        check_vma=False,
    )
```

```python
import functools

import jax
import jax.numpy as jnp
from jax import lax
from jax.experimental import pallas as pl
from jax.experimental.pallas import tpu as pltpu
from jax.sharding import PartitionSpec as P


def swapped_2(value, axis, apart):
    mask = 2**apart
    pairs = [(source, source ^ mask) for source in range(lax.axis_size(axis))]
    return lax.ppermute(value, axis, pairs)


def slot_table(routes, experts, capacity):
    local_tokens, choices = routes.shape
    expert_ids = routes.reshape(-1)
    one_hot = (expert_ids[:, None] == jnp.arange(experts, dtype=jnp.int32)[None, :]).astype(
        jnp.int32
    )
    earlier = jnp.cumsum(one_hot, axis=0) - one_hot
    slots = jnp.sum(earlier * one_hot, axis=1)
    position = expert_ids * capacity + slots
    source_token = jnp.arange(local_tokens * choices, dtype=jnp.int32) // choices
    token_table = jnp.zeros((experts * capacity,), jnp.int32).at[position].set(source_token)
    return (expert_ids, slots, token_table.reshape(experts, capacity))


def contract_width(rows, weight):
    return lax.dot_general(
        rows, weight, (((2,), (1,)), ((), ())), preferred_element_type=jnp.float32
    )


def slot_shards(expert_down, out_grad, routes, gates):
    devices = lax.axis_size("expert")
    experts = devices // 2
    local_tokens, choices = routes.shape
    hidden_half = expert_down.shape[0]
    capacity = 3 * local_tokens * choices // (2 * experts)
    expert_ids, slots, token_table = slot_table(routes, experts, capacity)
    parity = lax.axis_index("expert") % 2
    swapped = swapped_2(expert_down, "expert", 0)
    first_rows = jnp.where(parity == 0, expert_down, swapped)
    second_rows = jnp.where(parity == 0, swapped, expert_down)
    half_capacity = capacity // 2
    dispatch_order = token_table.reshape(experts, half_capacity, 2).transpose(0, 2, 1)
    outgoing = out_grad[dispatch_order.reshape(devices, half_capacity)]
    arrived = lax.all_to_all(outgoing, "expert", split_axis=0, concat_axis=0, tiled=True)
    low_part = contract_width(arrived, first_rows).astype(jnp.bfloat16)
    high_part = contract_width(arrived, second_rows).astype(jnp.bfloat16)
    product = jnp.concatenate([low_part, high_part], axis=2)
    returned = lax.all_to_all(product, "expert", split_axis=0, concat_axis=0, tiled=True)
    picked = returned.reshape(experts, 2, half_capacity, 2 * hidden_half)[
        expert_ids, slots % 2, slots // 2, :
    ]
    result = (gates.reshape(-1)[:, None] * picked.astype(jnp.float32)).astype(jnp.bfloat16)
    return result.reshape(local_tokens, choices, 2 * hidden_half)


VMEM = pl.BlockSpec(memory_space=pltpu.VMEM)


def columns(table):
    choices, count = table.shape
    padded = jnp.concatenate([table, jnp.zeros((-choices % 8, count), table.dtype)], axis=0)
    return padded.T[:, :choices]


def multiply_body(groups, steps, chips, has_kept, *refs):
    slots = len(steps)
    token_refs = refs[:groups]
    route_refs = refs[groups : 2 * groups]
    weight_refs = refs[2 * groups : 2 * groups + 2 * slots]
    at = 2 * groups + 2 * slots
    kept_refs = refs[at : at + groups] if has_kept else None
    at += groups if has_kept else 0
    out_refs = refs[at : at + groups]
    all_tokens, all_rows = refs[at + groups :]
    count = token_refs[0].shape[0]
    piece = weight_refs[0].shape[0]
    choices = route_refs[0].shape[0]
    for g in range(groups):
        all_tokens[g * count : (g + 1) * count, :] = token_refs[g][...]
    for at, rows in enumerate(weight_refs):
        all_rows[at * piece : (at + 1) * piece, :] = rows[...]
    value = lax.dot_general(
        all_tokens[...], all_rows[...], (((1,), (1,)), ((), ())), preferred_element_type=jnp.float32
    )
    chip = lax.axis_index("expert") // 2
    span = 2 * piece
    for g in range(groups):
        named = columns(route_refs[g][...])
        for j in range(choices):
            if has_kept:
                kept = kept_refs[g][:, j * span : (j + 1) * span].astype(jnp.float32)
            else:
                kept = jnp.zeros((count, span), jnp.float32)
            for s, step in enumerate(steps):
                expert = lax.rem(chip + step + chips, chips)
                part = value[g * count : (g + 1) * count, s * span : (s + 1) * span]
                kept = jnp.where(named[:, j : j + 1] == expert, part, kept)
            out_refs[g][:, j * span : (j + 1) * span] = kept.astype(jnp.bfloat16)


def multiply(steps, chips, tokens, routes, weights, kept=None):
    groups, slots = len(tokens), len(weights)
    rows, width = tokens[0].shape
    piece = weights[0][0].shape[0]
    choices = routes[0].shape[0]
    operands = [*tokens, *routes]
    for low, high in weights:
        operands += [low, high]
    if kept is not None:
        operands += kept
    shape = jax.ShapeDtypeStruct((rows, choices * 2 * piece), jnp.bfloat16)
    return pl.pallas_call(
        functools.partial(multiply_body, groups, steps, chips, kept is not None),
        out_shape=[shape] * groups,
        in_specs=[VMEM] * len(operands),
        out_specs=[VMEM] * groups,
        scratch_shapes=[
            pltpu.VMEM((groups * rows, width), jnp.bfloat16),
            pltpu.VMEM((slots * 2 * piece, width), jnp.bfloat16),
        ],
        compiler_params=pltpu.CompilerParams(vmem_limit_bytes=24 * 2**20),
        cost_estimate=pl.CostEstimate(
            flops=2 * groups * rows * slots * 2 * piece * width,
            bytes_accessed=2 * (groups * rows * width + slots * 2 * piece * width),
            transcendentals=0,
        ),
        name=f"multiply_{groups}_{slots}_{'late' if kept is not None else 'early'}",
    )(*operands)


def assemble_body(replicas, *refs):
    back_refs, gates_ref, out_ref, held = refs[:replicas], *refs[replicas:]
    choices = gates_ref.shape[0]
    span = back_refs[0].shape[1] // choices
    piece = span // 2
    replica = lax.axis_index("dp")
    core = lax.axis_index("expert") % 2
    for mask in range(replicas):
        held[mask] = back_refs[mask][...]
    gates = columns(gates_ref[...])
    picked = []
    for j in range(choices):
        lows, highs = [], []
        for source in range(replicas):
            value = held[replica ^ source, :, j * span : (j + 1) * span].astype(jnp.float32)
            own, other = value[:, :piece], value[:, piece:]
            lows.append(jnp.where(core == 0, own, other))
            highs.append(jnp.where(core == 0, other, own))
        row = jnp.concatenate(lows + highs, axis=1) * gates[:, j : j + 1]
        picked.append(row.astype(jnp.bfloat16))
    for j in range(choices):
        out_ref[:, j, :] = picked[j]


def assemble(back, gates):
    rows, columns_each = back[0].shape
    choices = gates.shape[0]
    replicas = len(back)
    return pl.pallas_call(
        functools.partial(assemble_body, replicas),
        out_shape=jax.ShapeDtypeStruct((rows, choices, replicas * columns_each // choices), jnp.bfloat16),
        in_specs=[VMEM] * (replicas + 1),
        out_specs=VMEM,
        scratch_shapes=[pltpu.VMEM((replicas, rows, columns_each), jnp.bfloat16)],
        compiler_params=pltpu.CompilerParams(vmem_limit_bytes=16 * 2**20),
        name="assemble",
    )(*back, gates)


def piece_shards(expert_down, out_grad, routes, gates):
    devices = lax.axis_size("expert")
    replicas = lax.axis_size("dp")
    chips = devices // 2
    hidden_half, width = expert_down.shape
    piece = hidden_half // replicas
    replica = lax.axis_index("dp")

    def along(value, by):
        return lax.ppermute(value, "expert", [(i, (i + 2 * by) % devices) for i in range(devices)])

    def other_core(value):
        return lax.ppermute(value, "expert", [(i, i ^ 1) for i in range(devices)])

    def other_replica(value, mask):
        return lax.ppermute(value, "dp", [(i, i ^ mask) for i in range(replicas)])

    mine = lax.dynamic_slice(expert_down, (replica * piece, 0), (piece, width))
    ups, downs = [mine], [mine]
    for _ in range(chips // 2):
        ups.append(along(ups[-1], 1))
    for _ in range((chips - 1) // 2):
        downs.append(along(downs[-1], -1))
    held = [(0, mine)]
    for step in range(1, chips // 2 + 1):
        if step < len(downs):
            held.append((step, downs[step]))
        held.append((-step, ups[step]))
    steps = [step for step, _ in held]
    weights = [(rows, other_core(rows)) for _, rows in held]

    named = routes.T
    tokens = [out_grad] + [other_replica(out_grad, mask) for mask in range(1, replicas)]
    named = [named] + [other_replica(named, mask) for mask in range(1, replicas)]
    early = multiply(steps[:-1], chips, tokens, named, weights[:-1])
    late = multiply(steps[-1:], chips, tokens, named, weights[-1:], early)
    back = [late[0]] + [other_replica(late[mask], mask) for mask in range(1, replicas)]
    return assemble(back, gates.T)


def shards(expert_down, out_grad, routes, gates):
    experts, replicas = lax.axis_size("expert") // 2, lax.axis_size("dp")
    shared = experts <= replicas and replicas & (replicas - 1) == 0
    shared = shared and expert_down.shape[0] % (16 * replicas) == 0
    plan = piece_shards if shared else slot_shards
    return plan(expert_down, out_grad, routes, gates)


def solution(mesh):
    placed = (
        P("expert", None),
        P(("dp", "expert"), None),
        P(("dp", "expert"), None),
        P(("dp", "expert"), None),
    )
    return jax.shard_map(
        shards,
        mesh=mesh,
        in_specs=placed,
        out_specs=P(("dp", "expert"), None, None),
        check_vma=False,
    )
```
